64 devices in a mesh: dp: 4 (over x, y), sp: 16 (over z, core).
Axes of the slice: x: 2, y: 2, z: 8, core: 2. Of those that a mesh axis runs over, the one named last changes fastest.
The devices are a block of a 4x4x8 slice.
Arguments:
- x_steps: bfloat16 [4, 64, 2560], P(None, 'dp'), parts along dimension 1
- k_cache: bfloat16 [64, 2048, 8, 128], P('dp', 'sp'), parts along dimension 0
- v_cache: bfloat16 [64, 2048, 8, 128], P('dp', 'sp'), parts along dimension 0
- seq_lens: int32 [64], P('dp'), parts along dimension 0
- norm_gain: bfloat16 [2560], replicated
- w_q: bfloat16 [2560, 4096], replicated
- w_k: bfloat16 [2560, 1024], replicated
- w_v: bfloat16 [2560, 1024], replicated
- w_o: bfloat16 [4096, 2560], replicated
- q_gain: bfloat16 [128], replicated
- k_gain: bfloat16 [128], replicated
Outputs:
- output 1: bfloat16 [4, 64, 2560], P(None, 'dp'), parts along dimension 1
- output 2: bfloat16 [64, 2048, 8, 128], P('dp', 'sp'), parts along dimension 0
- output 3: bfloat16 [64, 2048, 8, 128], P('dp', 'sp'), parts along dimension 0
There are 4 independent parts. The reference program is written for one: setup_inputs(seed, part) draws one part's arguments, and reference() takes and returns one part's arrays. A program takes and returns all parts, laid end to end along the dimension named above; an argument that names none is the same for every part.
All inputs are finite; a program needn't handle non-finite values.
Results may differ from the reference program's by a relative error of at most 0.0108835.
Values sent between devices are 32-bit elements.
A program may use at most 768 MiB of HBM per device.

```python
import math
import jax
import jax.numpy as jnp
from jax import lax

STEPS = 4
BATCH = 16
SEQ_LEN = 2048
HIDDEN = 2560
NUM_Q_HEADS = 32
NUM_KV_HEADS = 8
HEAD_DIM = 128
ROPE_BASE = 1000000
NORM_EPS = 1e-6


def draw_lengths(key):
    keys = jax.random.split(key, 3)
    lengths = jax.random.randint(keys[0], (BATCH,), 0, SEQ_LEN - STEPS + 1, dtype=jnp.int32)
    order = jax.random.permutation(keys[1], BATCH)
    short_count = max(1, BATCH // 4)
    lengths = lengths.at[order[0]].set(SEQ_LEN - STEPS)
    short_lens = jax.random.randint(keys[2], (short_count,), 0, 16, dtype=jnp.int32)
    return lengths.at[order[1:1 + short_count]].set(short_lens)


def setup_inputs(seed: int = 0, part: int = 0) -> dict:
    shared = jax.random.split(jax.random.key(seed), 7)
    own_keys = jax.random.split(jax.random.fold_in(jax.random.key(seed + 1), part), 4)
    q_dim = NUM_Q_HEADS * HEAD_DIM
    kv_dim = NUM_KV_HEADS * HEAD_DIM
    score_scale = math.sqrt(math.log(SEQ_LEN / 16))
    cache_shape = (BATCH, SEQ_LEN, NUM_KV_HEADS, HEAD_DIM)

    def normal(key, shape):
        return jax.random.normal(key, shape, jnp.float32)

    return {
        'x_steps': (0.5 * normal(own_keys[0], (STEPS, BATCH, HIDDEN))).astype(jnp.bfloat16),
        'k_cache': normal(own_keys[1], cache_shape).astype(jnp.bfloat16),
        'v_cache': normal(own_keys[2], cache_shape).astype(jnp.bfloat16),
        'seq_lens': draw_lengths(own_keys[3]),
        'norm_gain': (1.0 + 0.3 * normal(shared[0], (HIDDEN,))).astype(jnp.bfloat16),
        'w_q': (normal(shared[1], (HIDDEN, q_dim)) * HIDDEN ** -0.5).astype(jnp.bfloat16),
        'w_k': (normal(shared[2], (HIDDEN, kv_dim)) * HIDDEN ** -0.5).astype(jnp.bfloat16),
        'w_v': (normal(shared[3], (HIDDEN, kv_dim)) * HIDDEN ** -0.5).astype(jnp.bfloat16),
        'w_o': (normal(shared[4], (q_dim, HIDDEN)) * q_dim ** -0.5).astype(jnp.bfloat16),
        'q_gain': (score_scale * (1.0 + 0.2 * normal(shared[5], (HEAD_DIM,)))).astype(jnp.bfloat16),
        'k_gain': (1.0 + 0.2 * normal(shared[6], (HEAD_DIM,))).astype(jnp.bfloat16),
    }


def rms_scale(values, gain):
    inv_rms = lax.rsqrt(jnp.mean(values * values, axis=-1, keepdims=True) + NORM_EPS)
    return values * inv_rms * gain.astype(jnp.float32)


def rope_rotate(values, positions):
    half_dim = HEAD_DIM // 2
    inv_freq = jnp.exp(jnp.arange(half_dim, dtype=jnp.float32) * (-2.0 * math.log(ROPE_BASE) / HEAD_DIM))
    angles = positions.astype(jnp.float32)[..., None, None] * inv_freq
    cosine = jnp.cos(angles)
    sine = jnp.sin(angles)
    lower_half = values[..., :half_dim]
    upper_half = values[..., half_dim:]
    return jnp.concatenate([lower_half * cosine - upper_half * sine, upper_half * cosine + lower_half * sine], axis=-1)


def reference(x_steps, k_cache, v_cache, seq_lens, norm_gain, w_q, w_k, w_v, w_o, q_gain, k_gain):
    group = NUM_Q_HEADS // NUM_KV_HEADS
    slot_ids = jnp.arange(SEQ_LEN)
    rows = jnp.arange(BATCH)

    def attend_one(operands):
        query, keys, vals, position = operands
        grouped = query.reshape(NUM_KV_HEADS, group, HEAD_DIM).astype(jnp.float32)
        scores = jnp.einsum('kgd,skd->kgs', grouped, keys.astype(jnp.float32)) * HEAD_DIM ** -0.5
        scores = jnp.where((slot_ids <= position)[None, None, :], scores, -jnp.inf)
        weights = jax.nn.softmax(scores, axis=-1)
        mixed = jnp.einsum('kgs,skd->kgd', weights, vals.astype(jnp.float32))
        return mixed.reshape(NUM_Q_HEADS, HEAD_DIM)

    def decode_step(caches, step_in):
        k_now, v_now = caches
        x_now, step = step_in
        positions = seq_lens + step
        x_f32 = x_now.astype(jnp.float32)
        normed = rms_scale(x_f32, norm_gain).astype(jnp.bfloat16)
        queries = jnp.dot(normed, w_q, preferred_element_type=jnp.float32).astype(jnp.bfloat16)
        keys_new = jnp.dot(normed, w_k, preferred_element_type=jnp.float32).astype(jnp.bfloat16)
        vals_new = jnp.dot(normed, w_v, preferred_element_type=jnp.float32).astype(jnp.bfloat16)
        queries = queries.reshape(BATCH, NUM_Q_HEADS, HEAD_DIM)
        keys_new = keys_new.reshape(BATCH, NUM_KV_HEADS, HEAD_DIM)
        vals_new = vals_new.reshape(BATCH, NUM_KV_HEADS, HEAD_DIM)
        queries = rope_rotate(rms_scale(queries.astype(jnp.float32), q_gain), positions).astype(jnp.bfloat16)
        keys_new = rope_rotate(rms_scale(keys_new.astype(jnp.float32), k_gain), positions).astype(jnp.bfloat16)
        k_now = k_now.at[rows, positions].set(keys_new)
        v_now = v_now.at[rows, positions].set(vals_new)
        attended = lax.map(attend_one, (queries, k_now, v_now, positions)).astype(jnp.bfloat16)
        out_proj = jnp.dot(attended.reshape(BATCH, -1), w_o, preferred_element_type=jnp.float32)
        y_now = (x_f32 + out_proj).astype(jnp.bfloat16)
        return (k_now, v_now), y_now

    (k_out, v_out), y_steps = lax.scan(decode_step, (k_cache, v_cache), (x_steps, jnp.arange(STEPS)))
    return (y_steps, k_out, v_out)
```

```python
import functools
import math
import jax
import jax.numpy as jnp
from jax import lax
from jax.experimental import pallas as pl
from jax.experimental.pallas import tpu as pltpu
from jax.sharding import PartitionSpec as P

NORM_EPS = 1e-6
ROPE_BASE = 1000000.0
MESH = pl.DeviceIdType.MESH
NEG = -1e30
COLS = 512
ROWS = 16
MSG = 8
VMEM_LIMIT = 67043328


def attend_kernel(dims, lens, x_ref, gain_ref, qg_ref, kg_ref, wq_hbm, wk_hbm, wv_hbm, kc_hbm, vc_hbm,
                  part_ref, ko_hbm, vo_hbm,
                  wbuf, kbuf, vbuf, h_ref, cos_ref, sin_ref, q_rows, k_rows, v_rows, colid, s_buf, p_buf,
                  w_sem, k_sem, v_sem, ko_sem, vo_sem):
    steps, batch, slots, kv_heads, head_dim, q_heads = dims
    group = q_heads // kv_heads
    half_heads = q_heads // 2
    rows = steps * batch
    kv_cols = kv_heads * head_dim // COLS
    q_cols = q_heads * head_dim // COLS
    per_chunk = COLS // head_dim
    first_slot = lax.axis_index('sp') * slots

    def weight_copy(index, source, column):
        return pltpu.make_async_copy(source.at[:, pl.ds(column * COLS, COLS)], wbuf.at[index], w_sem.at[index])

    def cache_copy(b, source, target, sems):
        return pltpu.make_async_copy(source.at[b], target.at[b], sems.at[b])

    for i in range(kv_cols):
        weight_copy(i, wk_hbm, i).start()
    for i in range(kv_cols):
        weight_copy(kv_cols + i, wv_hbm, i).start()
    for b in range(batch):
        cache_copy(b, kc_hbm, kbuf, k_sem).start()
        cache_copy(b, vc_hbm, vbuf, v_sem).start()
    for i in range(q_cols):
        weight_copy(2 * kv_cols + i, wq_hbm, i).start()

    x = x_ref[...].astype(jnp.float32)
    inv = lax.rsqrt(jnp.mean(x * x, axis=-1, keepdims=True) + NORM_EPS)
    h_ref[...] = (x * inv * gain_ref[...].astype(jnp.float32)).astype(jnp.bfloat16)

    row = lax.broadcasted_iota(jnp.int32, (rows, head_dim), 0)
    lane = lax.broadcasted_iota(jnp.int32, (rows, head_dim), 1)
    position = row // batch
    for b in range(batch):
        position = position + jnp.where(row % batch == b, lens[b], 0)
    half_dim = head_dim // 2
    freq = jnp.exp((lane % half_dim).astype(jnp.float32) * (-2.0 * math.log(ROPE_BASE) / head_dim))
    angle = position.astype(jnp.float32) * freq
    cos_ref[...] = jnp.cos(angle)
    sine = jnp.sin(angle)
    sin_ref[...] = jnp.where(lane < half_dim, -sine, sine)

    col = lax.broadcasted_iota(jnp.int32, (ROWS, slots * kv_heads), 1)
    head = lax.broadcasted_iota(jnp.int32, (ROWS, slots * kv_heads), 0)
    for half in range(2):
        match = (half * half_heads + head) // group == col % kv_heads
        colid[half] = jnp.where(match, col, jnp.int32(2 ** 30))

    def head_norm(values, gain):
        inv = lax.rsqrt(jnp.mean(values * values, axis=-1, keepdims=True) + NORM_EPS)
        values = values * inv * gain
        return values * cos_ref[...] + pltpu.roll(values, half_dim, 1) * sin_ref[...]

    def project(index):
        out = jnp.dot(h_ref[...], wbuf[index], preferred_element_type=jnp.float32)
        return out.astype(jnp.bfloat16).astype(jnp.float32)

    kg = kg_ref[...].astype(jnp.float32)
    qg = qg_ref[...].astype(jnp.float32)
    for i in range(kv_cols):
        weight_copy(i, wk_hbm, i).wait()
        out = project(i)
        for n in range(per_chunk):
            k_rows[pl.ds(i * per_chunk + n, rows, stride=kv_heads), :] = head_norm(out[:, n * head_dim:(n + 1) * head_dim], kg)
    for i in range(kv_cols):
        weight_copy(kv_cols + i, wv_hbm, i).wait()
        out = project(kv_cols + i)
        for n in range(per_chunk):
            v_rows[pl.ds(i * per_chunk + n, rows, stride=kv_heads), :] = out[:, n * head_dim:(n + 1) * head_dim]

    def update(b, _):
        cache_copy(b, kc_hbm, kbuf, k_sem).wait()
        cache_copy(b, vc_hbm, vbuf, v_sem).wait()
        for t in range(steps):
            slot = lens[b] + t - first_slot

            @pl.when((slot >= 0) & (slot < slots))
            def _():
                start = pl.multiple_of(slot // 2 * 2 * kv_heads, 2 * kv_heads)
                upper = lax.broadcasted_iota(jnp.int32, (2 * kv_heads, head_dim), 0) // kv_heads
                for buf, new in ((kbuf, k_rows), (vbuf, v_rows)):
                    fresh = new[pl.ds(pl.multiple_of((t * batch + b) * kv_heads, kv_heads), kv_heads), :]
                    fresh = jnp.concatenate([fresh, fresh], axis=0)
                    old = buf[b, pl.ds(start, 2 * kv_heads), :].astype(jnp.float32)
                    buf[b, pl.ds(start, 2 * kv_heads), :] = jnp.where(upper == slot % 2, fresh, old).astype(jnp.bfloat16)
        return 0

    lax.fori_loop(0, batch, update, 0)

    def project_q(i, _):
        weight_copy(2 * kv_cols + i, wq_hbm, i).wait()
        out = project(2 * kv_cols + i)
        for n in range(per_chunk):
            q_rows[pl.ds(i * per_chunk + n, rows, stride=q_heads), :] = head_norm(out[:, n * head_dim:(n + 1) * head_dim], qg)
        return 0

    lax.fori_loop(0, q_cols, project_q, 0)

    def write_back(b, _):
        cache_copy(b, kbuf, ko_hbm, ko_sem).start()
        cache_copy(b, vbuf, vo_hbm, vo_sem).start()
        return 0

    lax.fori_loop(0, batch, write_back, 0)

    scale = head_dim ** -0.5 * math.log2(math.e)

    def scores(b, place):
        q = []
        for half in range(2):
            for t in range(steps):
                start = pl.multiple_of((t * batch + b) * q_heads + half * half_heads, half_heads)
                q.append(q_rows[pl.ds(start, half_heads), :].astype(jnp.bfloat16))
        q = jnp.concatenate(q, axis=0)
        s_buf[place] = lax.dot_general(q, kbuf[b], (((1,), (1,)), ((), ())), preferred_element_type=jnp.float32)

    def soften(b, place):
        diag_lane = lax.broadcasted_iota(jnp.int32, (ROWS, head_dim), 1)
        diag_row = lax.broadcasted_iota(jnp.int32, (ROWS, head_dim), 0)
        sub = lax.broadcasted_iota(jnp.int32, (MSG, head_dim), 0)
        for half in range(2):
            max_sum = jnp.zeros((ROWS, head_dim), jnp.float32)
            den_sum = jnp.zeros((ROWS, head_dim), jnp.float32)
            for t in range(steps):
                r0 = (half * steps + t) * ROWS
                limit = (lens[b] + t - first_slot + 1) * kv_heads
                s = jnp.where(colid[half] < limit, s_buf[place, r0:r0 + ROWS, :] * scale, -jnp.inf)
                top = jnp.maximum(jnp.max(s, axis=-1, keepdims=True), NEG)
                p = jnp.exp2(s - top)
                den = jnp.sum(p, axis=-1, keepdims=True)
                p_buf[place, r0:r0 + ROWS, :] = p.astype(jnp.bfloat16)
                own = diag_lane == diag_row + t * ROWS
                max_sum = max_sum + jnp.where(own, top, 0.0)
                den_sum = den_sum + jnp.where(own, den, 0.0)
            max_row = jnp.sum(max_sum, axis=0, keepdims=True)
            den_row = jnp.sum(den_sum, axis=0, keepdims=True)
            stats = jnp.where(sub == 0, max_row, jnp.where(sub == 1, den_row, 0.0))
            part_ref[half, b, steps * half_heads:, :] = stats

    def mix(b, place):
        out = jnp.dot(p_buf[place], vbuf[b], preferred_element_type=jnp.float32)
        for half in range(2):
            part_ref[half, b, :steps * half_heads, :] = out[half * steps * half_heads:(half + 1) * steps * half_heads]

    def attend(i, _):
        for place in range(2):
            scores(2 * i + place, place)
        for place in range(2):
            soften(2 * i + place, place)
        for place in range(2):
            mix(2 * i + place, place)
        return 0

    lax.fori_loop(0, batch // 2, attend, 0)

    def finish(b, _):
        cache_copy(b, kbuf, ko_hbm, ko_sem).wait()
        cache_copy(b, vbuf, vo_hbm, vo_sem).wait()
        return 0

    lax.fori_loop(0, batch, finish, 0)


def combine_kernel(dims, part_ref, x_ref, wo_hbm, y_ref,
                   wbuf, pair_in, own, out_s4, out_3, in_s4, in_3, in_f1, in_f2, fin, half_in, half_out,
                   mine, other,
                   w_sem, pair_send, pair_recv, rs_send, rs_recv, half_sem, ag_send, ag_recv, d2d_send, d2d_recv):
    steps, batch, q_heads, head_dim, hidden, chips = dims
    half_heads = q_heads // 2
    per_chip = batch // chips
    body = steps * half_heads
    msg = body + MSG
    half_cols = hidden // 2
    tiles = half_cols // head_dim
    block = per_chip * steps
    sp = lax.axis_index('sp')
    chip, core = sp // 2, sp % 2

    def chip_at(offset):
        return lax.rem(chip + offset + chips, chips)

    def device(offset):
        return {'sp': chip_at(offset) * 2 + core}

    partner = {'sp': chip * 2 + 1 - core}

    depth = q_heads * head_dim // 2
    parts = 4
    piece = depth // parts

    def weight_copy(i):
        start = pl.multiple_of(core * depth + i * piece, piece)
        return pltpu.make_async_copy(wo_hbm.at[pl.ds(start, piece), :], wbuf.at[i], w_sem.at[i])

    for i in range(parts):
        weight_copy(i).start()

    barrier = pltpu.get_barrier_semaphore()
    pl.semaphore_signal(barrier, inc=1, device_id=partner, device_id_type=MESH)
    for offset in (1, -1, 2, -2):
        pl.semaphore_signal(barrier, inc=1, device_id=device(offset), device_id_type=MESH)
    pl.semaphore_wait(barrier, 5)

    order = (4, 3, -3, 1, -1, 2, -2, 0)

    def pair_copy(i):
        start = pl.multiple_of(chip_at(order[i]) * per_chip, per_chip)
        return pltpu.make_async_remote_copy(
            src_ref=part_ref.at[1 - core, pl.ds(start, per_chip)], dst_ref=pair_in.at[i],
            send_sem=pair_send.at[i], recv_sem=pair_recv.at[i], device_id=partner, device_id_type=MESH)

    for i in range(len(order)):
        pair_copy(i).start()

    lane = lax.broadcasted_iota(jnp.int32, (body, head_dim), 1)
    row = lax.broadcasted_iota(jnp.int32, (body, head_dim), 0)
    diag = lane == row
    sub = lax.broadcasted_iota(jnp.int32, (MSG, head_dim), 0)

    def column(values):
        return jnp.sum(jnp.where(diag, values, 0.0), axis=-1, keepdims=True)

    def merge(pieces, last=False):
        tops = [p[body:body + 1, :] for p in pieces]
        dens = [p[body + 1:body + 2, :] for p in pieces]
        top = functools.reduce(jnp.maximum, tops)
        factors = [jnp.exp2(t - top) for t in tops]
        den = sum(f * d for f, d in zip(factors, dens))
        if last:
            factors = [f / den for f in factors]
        out = sum(column(f) * p[:body, :] for f, p in zip(factors, pieces))
        return out, jnp.where(sub == 0, top, jnp.where(sub == 1, den, 0.0))

    def reduce_into(target, pieces):
        out, stats = merge(pieces)
        target[:body, :] = out
        target[body:, :] = stats

    def mine_of(i, j):
        return part_ref.at[core, chip_at(order[i]) * per_chip + j]

    sends = []

    def send(src, dst, index, offset):
        copy = pltpu.make_async_remote_copy(
            src_ref=src, dst_ref=dst, send_sem=rs_send.at[index], recv_sem=rs_recv.at[index],
            device_id=device(offset), device_id_type=MESH)
        copy.start()
        sends.append(copy)
        return copy

    def pair_merge(i, target):
        pair_copy(i).wait_recv()
        for j in range(per_chip):
            reduce_into(target.at[j], [mine_of(i, j), pair_in.at[i, j]])

    pair_merge(0, out_s4)
    far = [send(out_s4.at[j], in_s4.at[j], j, 2 if j == 0 else -2) for j in range(per_chip)]
    third = []
    for d, sign in enumerate((1, -1)):
        pair_merge(1 + d, out_3.at[d])
        third.append([send(out_3.at[d, j], in_3.at[d, j], 2 + 2 * d + j, sign) for j in range(per_chip)])
    first = []
    for d, sign in enumerate((1, -1)):
        pair_merge(3 + d, own.at[d])
        first.append([send(own.at[d, j], in_f1.at[d, j], 6 + 2 * d + j, sign) for j in range(per_chip)])
    second = []
    for d, sign in enumerate((1, -1)):
        pair_copy(5 + d).wait_recv()
        second.append([])
    for j in range(per_chip):
        for d, sign in enumerate((1, -1)):
            pieces = [mine_of(5 + d, j), pair_in.at[5 + d, j]]
            third[d][j].wait_recv()
            pieces.append(in_3.at[d, j])
            if j == d:
                far[j].wait_recv()
                pieces.append(in_s4.at[j])
            reduce_into(own.at[2 + d, j], pieces)
            second[d].append(send(own.at[2 + d, j], in_f2.at[d, j], 10 + 2 * d + j, 2 * sign))
    pair_copy(7).wait_recv()
    for j in range(per_chip):
        pieces = [mine_of(7, j), pair_in.at[7, j]]
        for d in range(2):
            first[d][j].wait_recv()
            pieces.append(in_f1.at[d, j])
        for d in range(2):
            second[d][j].wait_recv()
            pieces.append(in_f2.at[d, j])
        fin[j * body:(j + 1) * body, :] = merge(pieces, last=True)[0]

    o = jnp.concatenate([fin[pl.ds(n, block, stride=half_heads), :] for n in range(half_heads)], axis=1).astype(jnp.bfloat16)
    acc = None
    for i in range(parts):
        weight_copy(i).wait()
        term = jnp.dot(o[:, i * piece:(i + 1) * piece], wbuf[i], preferred_element_type=jnp.float32)
        acc = term if acc is None else acc + term

    for n in range(tiles):
        left = acc[:, n * head_dim:(n + 1) * head_dim]
        right = acc[:, half_cols + n * head_dim:half_cols + (n + 1) * head_dim]
        half_out[0, n] = jnp.where(core == 0, right, left)
        half_out[1, n] = jnp.where(core == 0, left, right)
    swap = pltpu.make_async_remote_copy(
        src_ref=half_out.at[0], dst_ref=half_in, send_sem=half_sem.at[0], recv_sem=half_sem.at[1],
        device_id=partner, device_id_type=MESH)
    swap.start()
    swap.wait_recv()

    def rows_of(offset):
        return pl.ds(pl.multiple_of(chip_at(offset) * block, block), block)

    for n in range(tiles):
        mine[n, rows_of(0), :] = (x_ref[core, n, rows_of(0), :] + half_out[1, n] + half_in[n]).astype(jnp.bfloat16).astype(jnp.float32)

    gathers = []

    def gather(offset, target, index, span=(0, tiles)):
        view = mine.at[span[0]:span[1], rows_of(offset), :]
        copy = pltpu.make_async_remote_copy(
            src_ref=view, dst_ref=view, send_sem=ag_send.at[index], recv_sem=ag_recv.at[index],
            device_id=device(target), device_id_type=MESH)
        copy.start()
        gathers.append(copy)
        return copy

    def forward(offset, index, span=(0, tiles)):
        copy = pltpu.make_async_remote_copy(
            src_ref=mine.at[span[0]:span[1], rows_of(offset), :], dst_ref=other.at[span[0]:span[1], rows_of(offset), :],
            send_sem=d2d_send.at[index], recv_sem=d2d_recv.at[index], device_id=partner, device_id_type=MESH)
        copy.start()
        return copy

    mid = tiles // 2
    spans = ((0, mid), (mid, tiles))
    direct2 = [gather(0, 2 * sign, d) for d, sign in enumerate((1, -1))]
    direct1 = [gather(0, sign, 2 + d) for d, sign in enumerate((1, -1))]
    moved = [forward(0, 0)]
    relay4, relay3 = [], []
    for d, sign in enumerate((1, -1)):
        direct2[d].wait_recv()
        relay4.append(gather(-2 * sign, 2 * sign, 4 + d, spans[d]))
        relay3.append(gather(-2 * sign, sign, 6 + d))
        moved.append(forward(-2 * sign, 1 + d))
    for d, sign in enumerate((1, -1)):
        direct1[d].wait_recv()
        moved.append(forward(-sign, 3 + d))
    for d, sign in enumerate((1, -1)):
        relay3[d].wait_recv()
        moved.append(forward(-3 * sign, 5 + d))
    for d, sign in enumerate((1, -1)):
        relay4[d].wait_recv()
        moved.append(forward(-4 * sign, 7 + d, spans[d]))
    for copy in moved:
        copy.wait_recv()

    for n in range(tiles):
        for t in range(steps):
            here = mine[n, pl.ds(t, batch, stride=steps), :]
            there = other[n, pl.ds(t, batch, stride=steps), :]
            y_ref[t, :, n * head_dim:(n + 1) * head_dim] = jnp.where(core == 0, here, there).astype(jnp.bfloat16)
            y_ref[t, :, half_cols + n * head_dim:half_cols + (n + 1) * head_dim] = jnp.where(core == 0, there, here).astype(jnp.bfloat16)

    for i in range(len(order)):
        pair_copy(i).wait_send()
    for copy in sends + [swap] + gathers + moved:
        copy.wait_send()


def solution(mesh):
    chips = mesh.shape['sp'] // 2
    assert chips == 8

    def per_device(x_steps, k_local, v_local, seq_lens, norm_gain, w_q, w_k, w_v, w_o, q_gain, k_gain):
        steps, batch, hidden = x_steps.shape
        slots, kv_heads, head_dim = k_local.shape[1:]
        q_heads = w_q.shape[1] // head_dim
        half_heads = q_heads // 2
        rows = steps * batch
        msg = steps * half_heads + MSG
        assert half_heads == ROWS and batch == 2 * chips
        vmem = pl.BlockSpec(memory_space=pltpu.VMEM)
        hbm = pl.BlockSpec(memory_space=pltpu.HBM)
        smem = pl.BlockSpec(memory_space=pltpu.SMEM)
        chunks = (w_q.shape[1] + w_k.shape[1] + w_v.shape[1]) // COLS
        flat = (batch, slots * kv_heads, head_dim)
        bf16, f32 = jnp.bfloat16, jnp.float32
        part, k_new, v_new = pl.pallas_call(
            functools.partial(attend_kernel, (steps, batch, slots, kv_heads, head_dim, q_heads)),
            out_shape=(jax.ShapeDtypeStruct((2, batch, msg, head_dim), f32), jax.ShapeDtypeStruct(flat, bf16), jax.ShapeDtypeStruct(flat, bf16)),
            in_specs=[smem, vmem, vmem, vmem, vmem, hbm, hbm, hbm, hbm, hbm],
            out_specs=(vmem, hbm, hbm),
            scratch_shapes=[
                pltpu.VMEM((chunks, hidden, COLS), bf16), pltpu.VMEM(flat, bf16), pltpu.VMEM(flat, bf16),
                pltpu.VMEM((rows, hidden), bf16), pltpu.VMEM((rows, head_dim), f32), pltpu.VMEM((rows, head_dim), f32),
                pltpu.VMEM((rows * q_heads, head_dim), f32), pltpu.VMEM((rows * kv_heads, head_dim), f32),
                pltpu.VMEM((rows * kv_heads, head_dim), f32), pltpu.VMEM((2, ROWS, slots * kv_heads), jnp.int32),
                pltpu.VMEM((2, steps * q_heads, slots * kv_heads), f32), pltpu.VMEM((2, steps * q_heads, slots * kv_heads), bf16),
                pltpu.SemaphoreType.DMA((chunks,)), pltpu.SemaphoreType.DMA((batch,)), pltpu.SemaphoreType.DMA((batch,)),
                pltpu.SemaphoreType.DMA((batch,)), pltpu.SemaphoreType.DMA((batch,)),
            ],
            compiler_params=pltpu.CompilerParams(vmem_limit_bytes=VMEM_LIMIT),
            name='attend',
        )(seq_lens, x_steps.reshape(rows, hidden), norm_gain.reshape(1, -1), q_gain.reshape(1, -1), k_gain.reshape(1, -1),
          w_q, w_k, w_v, k_local.reshape(flat), v_local.reshape(flat))

        tiles = hidden // 2 // head_dim
        block = batch // chips * steps
        x_tiles = x_steps.astype(f32).reshape(steps, batch, 2, tiles, head_dim).transpose(2, 3, 1, 0, 4).reshape(2, tiles, rows, head_dim)
        pair = (batch // chips, msg, head_dim)
        sem = pltpu.SemaphoreType.DMA
        y_steps = pl.pallas_call(
            functools.partial(combine_kernel, (steps, batch, q_heads, head_dim, hidden, chips)),
            out_shape=jax.ShapeDtypeStruct(x_steps.shape, bf16),
            in_specs=[vmem, vmem, hbm],
            out_specs=vmem,
            scratch_shapes=[
                pltpu.VMEM((4, q_heads * head_dim // 8, hidden), bf16), pltpu.VMEM((8,) + pair, f32), pltpu.VMEM((4,) + pair, f32),
                pltpu.VMEM(pair, f32), pltpu.VMEM((2,) + pair, f32), pltpu.VMEM(pair, f32), pltpu.VMEM((2,) + pair, f32),
                pltpu.VMEM((2,) + pair, f32), pltpu.VMEM((2,) + pair, f32),
                pltpu.VMEM((batch // chips * steps * half_heads, head_dim), f32),
                pltpu.VMEM((tiles, block, head_dim), f32), pltpu.VMEM((2, tiles, block, head_dim), f32),
                pltpu.VMEM((tiles, rows, head_dim), f32), pltpu.VMEM((tiles, rows, head_dim), f32),
                sem((4,)), sem((8,)), sem((8,)), sem((14,)), sem((14,)), sem((2,)), sem((8,)), sem((8,)), sem((9,)), sem((9,)),
            ],
            compiler_params=pltpu.CompilerParams(vmem_limit_bytes=VMEM_LIMIT, collective_id=0, has_side_effects=True),
            name='combine',
        )(part, x_tiles, w_o)
        return y_steps, k_new.reshape(k_local.shape), v_new.reshape(v_local.shape)

    cache_spec = P('dp', 'sp', None, None)
    step_spec = P(None, 'dp', None)
    return jax.shard_map(per_device, mesh=mesh, in_specs=(step_spec, cache_spec, cache_spec, P('dp'), P(), P(), P(), P(), P(), P(), P()), out_specs=(step_spec, cache_spec, cache_spec), check_vma=False)
```
